256 devices in a mesh: tm: 64 (over z, x, core), blk: 4 (over y).
Axes of the slice: x: 4, y: 4, z: 8, core: 2. Of those that a mesh axis runs over, the one named last changes fastest.
Arguments:
- prior_mean: float32 [512], replicated, may hold values from -6 to 6
- after_mean: float32 [512], replicated, may hold values from -6 to 6
- filter_map: float32 [128, 512, 512], P('tm', 'blk'), may hold values from -1 to 1.5
- smoother_gain: float32 [128, 512, 512], P('tm', 'blk'), may hold values from -1 to 1.5
- smoother_map: float32 [128, 512, 512], P('tm', 'blk'), may hold values from -1 to 1.5
- obs_gain: float32 [128, 512, 128], P('tm', 'blk'), may hold values from -0.5 to 0.5
- observations: float32 [128, 128], P('tm'), may hold values from -6 to 6
Outputs:
- filtered: float32 [128, 512], P('tm', 'blk')
- smoothed: float32 [128, 512], P('tm', 'blk')
The draws below stay inside these ranges and needn't reach their ends.
All inputs are finite; a program needn't handle non-finite values.
Results may differ from the reference program's by a relative error of at most 0.0003.
Values sent between devices are 32-bit elements; how exact they have to be, the bound alone decides.
A program may use at most 128 MiB of HBM per device.

```python
import math
import jax
import jax.numpy as jnp
from jax import lax

LATENT_SIZE = 512
OBS = 128
HORIZON_LENGTH = 128


def decaying_map(key, lasting_share, mixing_size):
    sampler_seeds = jax.random.split(key, 7)
    lasting = jax.random.uniform(sampler_seeds[0], (LATENT_SIZE,)) < lasting_share
    fast_forget = jax.random.uniform(sampler_seeds[1], (LATENT_SIZE,), minval=0.06, maxval=0.12)
    slow_forget = jax.random.uniform(sampler_seeds[2], (LATENT_SIZE,), minval=0.01, maxval=0.025)
    forget = jnp.where(lasting, slow_forget, fast_forget)
    factor = jax.random.uniform(sampler_seeds[3], (HORIZON_LENGTH, LATENT_SIZE), minval=0.5, maxval=1.5)
    kept_entries = 1.0 - forget[None, :] * factor
    segment_batches = jax.random.randint(sampler_seeds[4], (3,), 0, HORIZON_LENGTH)
    segment_spacing = jnp.any(jnp.arange(HORIZON_LENGTH)[:, None] == segment_batches[None, :], axis=1)
    segment_limit = jax.random.uniform(sampler_seeds[5], (HORIZON_LENGTH, LATENT_SIZE), minval=0.5, maxval=0.8)
    kept_entries = jnp.where(segment_spacing[:, None], kept_entries * segment_limit, kept_entries)
    mixing = jax.random.truncated_normal(sampler_seeds[6], -4.0, 4.0, (HORIZON_LENGTH, LATENT_SIZE, LATENT_SIZE)) * (mixing_size / math.sqrt(LATENT_SIZE))
    return (mixing + kept_entries[:, :, None] * jnp.eye(LATENT_SIZE, dtype=jnp.float32)[None]).astype(jnp.float32)


def draw_filter_map(key, part):
    return decaying_map(jax.random.fold_in(key, 3), 0.5, 0.2)


def draw_smoother_gain(key, part):
    return decaying_map(jax.random.fold_in(key, 11), 0.5, 0.2)


def draw_smoother_map(key, part):
    sampler_seeds = jax.random.split(jax.random.fold_in(key, 19), 2)
    diagonal = jax.random.uniform(sampler_seeds[0], (HORIZON_LENGTH, LATENT_SIZE), minval=0.4, maxval=1.0)
    mixing = jax.random.truncated_normal(sampler_seeds[1], -4.0, 4.0, (HORIZON_LENGTH, LATENT_SIZE, LATENT_SIZE)) * (0.3 / math.sqrt(LATENT_SIZE))
    return (mixing + diagonal[:, :, None] * jnp.eye(LATENT_SIZE, dtype=jnp.float32)[None]).astype(jnp.float32)


def block_scale(rng, shape, cuts, least, high):
    level = 1.0
    for position, blocks in cuts:
        draws = jax.random.uniform(jax.random.fold_in(jax.random.fold_in(rng, 6), position), (blocks,), jnp.float32, least / len(cuts), high / len(cuts))
        level = level * jnp.repeat(jnp.exp(draws), shape[position] // blocks).reshape((-1,) + (1,) * (len(shape) - 1 - position))
    return level


def gaussian(stream_key, shape, spread, most, shards=(), kind=jnp.bfloat16):
    result = spread * jax.random.normal(stream_key, shape, jnp.float32)
    if shards:
        result = result * block_scale(stream_key, shape, shards, -0.22, 0.18)
    return jnp.clip(result, -most, most).astype(kind)


def setup_inputs(seed: int = 0) -> dict:
    arg_keys = jax.random.split(jax.random.key(seed), 8)
    return {
        "prior_mean": gaussian(arg_keys[0], (LATENT_SIZE,), 1.0, 6.0, (), jnp.float32),
        "after_mean": gaussian(arg_keys[1], (LATENT_SIZE,), 1.0, 6.0, (), jnp.float32),
        "filter_map": draw_filter_map(jax.random.fold_in(arg_keys[7], 71), 0),
        "smoother_gain": draw_smoother_gain(jax.random.fold_in(arg_keys[7], 71), 0),
        "smoother_map": draw_smoother_map(jax.random.fold_in(arg_keys[7], 71), 0),
        "obs_gain": gaussian(arg_keys[5], (HORIZON_LENGTH, LATENT_SIZE, OBS), OBS ** -0.5, 0.5, ((0, 64), (1, 4)), jnp.float32),
        "observations": gaussian(arg_keys[6], (HORIZON_LENGTH, OBS), 1.0, 6.0, ((0, 64),), jnp.float32),
    }


def reference(prior_mean, after_mean, filter_map, smoother_gain, smoother_map, obs_gain, observations):
    highest = lax.Precision.HIGHEST
    drive = jnp.einsum("tso,to->ts", obs_gain, observations, precision=highest)

    def forward(current, inputs):
        step_map, offset = inputs
        current = jnp.dot(step_map, current, precision=highest) + offset
        return current, current

    ignored, filtered = lax.scan(forward, prior_mean, (filter_map, drive))
    pulled = jnp.einsum("tsk,tk->ts", smoother_map, filtered, precision=highest)

    def backward(current, inputs):
        step_gain, offset = inputs
        current = jnp.dot(step_gain, current, precision=highest) + offset
        return current, current

    unused, smoothed = lax.scan(backward, after_mean, (smoother_gain, pulled), reverse=True)
    return filtered, smoothed
```

```python
import functools

import jax
import jax.numpy as jnp
from jax import lax
from jax.experimental import pallas as pl
from jax.experimental.pallas import tpu as pltpu
from jax.sharding import Mesh
from jax.sharding import PartitionSpec as P

TM = ("tm_0", "tm_1", "tm_2")
MESH = pl.DeviceIdType.MESH
R = 128
B = 4
Z = 8
HIGHEST = lax.Precision.HIGHEST


def mat(a, b):
    return jnp.dot(a, b, precision=HIGHEST, preferred_element_type=jnp.float32)


def spread(row):
    return jnp.broadcast_to(row, (R, R)).T


def row_dot(pairs):
    total = None
    for a, u in pairs:
        total = a * u if total is None else total + a * u
    return jnp.sum(total.T, axis=0, keepdims=True)


def fold(product):
    return jnp.sum(product.reshape(R // 8, 8, R), axis=0)


def cut(block, k):
    return block[:, k * R : (k + 1) * R]


def kernel(
    prior,
    after,
    filter_map,
    smoother_gain,
    smoother_map,
    obs_gain,
    observations,
    filtered_out,
    smoothed_out,
    full,
    last,
    help_rows,
    pull_map,
    gain,
    tails,
    prefix,
    columns,
    spreads,
    shift_spread,
    shifts,
    stage,
    drives,
    offsets,
    entering,
    middle,
    leaving,
    rows_out,
    states,
    smoothed_in,
    seen,
    load_sem,
    send_sem,
    full_sem,
    last_sem,
    drive_sem,
    column_sem,
    shift_y_sem,
    shift_x_sem,
    hop_sem,
    state_sem,
    smoothed_sem,
    gate_sem,
):
    z, x, y = lax.axis_index("tm_0"), lax.axis_index("tm_1"), lax.axis_index("blk")
    core = lax.axis_index("tm_2")

    def branch(c):
        forward = c == 0
        own = filter_map if forward else smoother_gain
        other = smoother_gain if forward else filter_map
        place = x if forward else B - 1 - x
        level = z if forward else Z - 1 - z
        sends = []

        def x_at(p):
            return p if forward else B - 1 - p

        def turn(i, d):
            return lax.rem(i + d, B)

        def back(i, d):
            return lax.rem(i + B - d, B)

        def rows(i):
            return pl.ds(pl.multiple_of(i * R, R), R)

        def remote(src, dst, recv, device):
            return pltpu.make_async_remote_copy(
                src_ref=src,
                dst_ref=dst,
                send_sem=send_sem.at[len(sends)],
                recv_sem=recv,
                device_id=device,
                device_id_type=MESH,
            )

        def send(src, dst, recv, device):
            copy = remote(src, dst, recv, device)
            copy.start()
            sends.append(copy)

        def arrive(dst, recv, device):
            pltpu.make_async_remote_copy(
                src_ref=dst,
                dst_ref=dst,
                send_sem=send_sem.at[0],
                recv_sem=recv,
                device_id=device,
                device_id_type=MESH,
            ).wait_recv()

        loads = []

        def load(src, dst):
            copy = pltpu.make_async_copy(src, dst, load_sem.at[len(loads)])
            copy.start()
            loads.append(copy)

        load(own.at[c], full.at[0, rows(y)])
        load(own.at[1 - c], full.at[1, rows(y)])
        load(other.at[1 - c], help_rows.at[0])
        load(other.at[c], help_rows.at[1])
        load(obs_gain, gain)
        load(observations, seen)
        load(smoother_map, pull_map)

        barrier = pltpu.get_barrier_semaphore()
        peers = [(z, x, c, turn(y, d)) for d in (1, 2, 3)]
        peers += [(z, x, 1 - c, turn(y, d)) for d in (0, 1, 2, 3)]
        peers += [(z, turn(x, d), c, y) for d in (1, 2, 3)]
        peers += [(lax.rem(z + 1, Z), x, c, y), (lax.rem(z + Z - 1, Z), x, c, y)]
        for peer in peers:
            pl.semaphore_signal(barrier, inc=1, device_id=peer, device_id_type=MESH)
        pl.semaphore_wait(barrier, len(peers))

        def send_own():
            for n in (1, 0):
                loads[n].wait()
                for d in (1, 3, 2):
                    mine = full.at[n, rows(y)]
                    send(mine, mine, full_sem.at[n, d], (z, x, c, turn(y, d)))

        def send_help():
            loads[2].wait()
            for d in (0, 1, 3, 2):
                send(
                    help_rows.at[0],
                    full.at[2, rows(y)],
                    full_sem.at[2, d],
                    (z, x, 1 - c, turn(y, d)),
                )
            loads[3].wait()
            send(help_rows.at[1], last, last_sem, (z, x, 1 - c, y))

        def share_drives(to, first):
            if to == c:
                drives[y, first : first + 2] = stage[first : first + 2]
            for d in (1, 3, 2) if to == c else (0, 1, 3, 2):
                send(
                    stage.at[first : first + 2],
                    drives.at[y, first : first + 2],
                    drive_sem.at[c, d],
                    (z, x, to, turn(y, d)),
                )

        def await_drives():
            for cc in (c, 1 - c):
                first = 2 * cc if forward else 2 - 2 * cc
                for d in (1, 3, 2) if cc == c else (0, 1, 3, 2):
                    i = back(y, d)
                    arrive(
                        drives.at[i, first : first + 2], drive_sem.at[cc, d], (z, x, cc, i)
                    )

        def compose():
            for d in (0, 1, 3, 2):
                i = back(y, d)
                arrive(full.at[2, rows(i)], full_sem.at[2, d], (z, x, 1 - c, i))
            arrive(last, last_sem, (z, x, 1 - c, y))
            tails[0] = mat(last[...], full[2])
            for d in (1, 3, 2):
                i = back(y, d)
                arrive(full.at[1, rows(i)], full_sem.at[1, d], (z, x, c, i))
            tails[1] = mat(tails[0], full[1])
            for d in (1, 3, 2):
                i = back(y, d)
                arrive(full.at[0, rows(i)], full_sem.at[0, d], (z, x, c, i))
            whole = mat(tails[1], full[0])
            turned = [cut(whole, k).T for k in range(B)]
            for k in range(B):
                prefix[3, k] = turned[k]

            @pl.when(lax.rem(place, 2) == 0)
            def _():
                for k in range(B):
                    columns[place, y, k] = cut(whole, k)

            @pl.when(lax.rem(place, 2) == 1)
            def _():
                for k in range(B):
                    columns[place, y, k] = turned[k]

        def half(p, i, h):
            return columns.at[p, i, 2 * h : 2 * h + 2]

        def to_y(p, dp, h):
            for d in (1, 3, 2):
                mine = half(p, y, h)
                send(mine, mine, column_sem.at[dp, d, h], (z, x, c, turn(y, d)))

        def to_x(i, di, h):
            for d in (1, 3, 2):
                mine = half(place, i, h)
                send(mine, mine, column_sem.at[d, di, h], (z, x_at(turn(place, d)), c, y))

        def share_columns():
            to_y(place, 0, 0)
            to_x(y, 0, 1)
            to_y(place, 0, 1)
            to_x(y, 0, 0)

        def finish_prefixes():
            mine = full[1, rows(y)]
            tails[2] = mat(full[2, rows(y)], full[1])
            first = mat(mine, full[0])
            second = mat(tails[2], full[0])
            zeroth = full[0, rows(y)]
            for k in range(B):
                prefix[0, k] = cut(zeroth, k).T
                prefix[1, k] = cut(first, k).T
                prefix[2, k] = cut(second, k).T

        def forward_columns():
            for d in (1, 3, 2):
                i = back(y, d)
                arrive(half(place, i, 0), column_sem.at[0, d, 0], (z, x, c, i))
                to_x(i, d, 0)
                p = back(place, d)
                arrive(half(p, y, 1), column_sem.at[d, 0, 1], (z, x_at(p), c, y))
                to_y(p, d, 1)

        def await_columns():
            for d in (1, 3, 2):
                i = back(y, d)
                arrive(half(place, i, 1), column_sem.at[0, d, 1], (z, x, c, i))
                p = back(place, d)
                arrive(half(p, y, 0), column_sem.at[d, 0, 0], (z, x_at(p), c, y))
            for dp in (1, 3, 2):
                p = back(place, dp)
                for d in (1, 3, 2):
                    i = back(y, d)
                    arrive(half(p, i, 0), column_sem.at[dp, d, 0], (z, x_at(p), c, y))
                    arrive(half(p, i, 1), column_sem.at[dp, d, 1], (z, x, c, i))

        def column_offsets():
            def d(i):
                return [drives[k, i] for k in range(B)]

            def pairs(block, i):
                return [(cut(block, k), u) for k, u in enumerate(d(i))]

            last_shift = row_dot(pairs(tails[1], 0) + pairs(tails[0], 1) + pairs(last[...], 2))
            last_shift = last_shift + drives[y, 3]
            offsets[3] = last_shift
            shifts[place, y] = last_shift
            for e in (1, 3, 2):
                send(
                    shifts.at[place, y],
                    shifts.at[place, y],
                    shift_y_sem.at[e],
                    (z, x, c, turn(y, e)),
                )
            third = row_dot(pairs(tails[2], 0) + pairs(full[2, rows(y)], 1))
            offsets[2] = third + drives[y, 2]
            offsets[1] = row_dot(pairs(full[1, rows(y)], 0)) + drives[y, 1]
            offsets[0] = drives[y, 0]
            for e in (1, 3, 2):
                i = back(y, e)
                arrive(shifts.at[place, i], shift_y_sem.at[e], (z, x, c, i))
            for e in (1, 3, 2):
                send(
                    shifts.at[place],
                    shifts.at[place],
                    shift_x_sem.at[e],
                    (z, x_at(turn(place, e)), c, y),
                )

        def await_shifts():
            for e in (1, 3, 2):
                p = back(place, e)
                arrive(shifts.at[p], shift_x_sem.at[e], (z, x_at(p), c, y))
            for n in range(2):
                for k in range(B):
                    shift_spread[n, k] = spread(shifts[2 * n, k])

        def pair(n, state):
            for i in range(B):
                total = None
                for k in range(B):
                    term = columns[2 * n, i, k] * state[k]
                    total = term if total is None else total + term
                reduced = jnp.sum(total, axis=1, keepdims=True)
                spreads[2 * n + 1, i] = jnp.broadcast_to(reduced, (R, R)) + shift_spread[n, i]
            result = []
            for i in range(B):
                total = None
                for k in range(B):
                    term = fold(columns[2 * n + 1, i, k] * spreads[2 * n + 1, k])
                    total = term if total is None else total + term
                result.append(jnp.sum(total, axis=0, keepdims=True) + shifts[2 * n + 1, i])
            return result

        def chain(start):
            up, down = (z + 1, z - 1) if forward else (z - 1, z + 1)

            @pl.when(level == 0)
            def _():
                entering[...] = start[...]

            @pl.when(level > 0)
            def _():
                arrive(entering, hop_sem, (down, x, c, y))

            state = pair(0, [entering[k] for k in range(B)])
            for k in range(B):
                middle[k] = state[k]
            state = pair(1, state)
            for k in range(B):
                leaving[k] = state[k]
            hop = remote(leaving, entering, hop_sem, (up, x, c, y))

            @pl.when(level < Z - 1)
            def _():
                hop.start()

            @pl.when(place == 0)
            def _():
                for k in range(B):
                    spreads[0, k] = spread(entering[k])

            @pl.when(place == 2)
            def _():
                for k in range(B):
                    spreads[2, k] = spread(middle[k])

            for i in range(4):
                total = None
                for k in range(B):
                    term = fold(prefix[i, k] * spreads[place, k])
                    total = term if total is None else total + term
                rows_out[i] = jnp.sum(total, axis=0, keepdims=True) + offsets[i]

            @pl.when(level < Z - 1)
            def _():
                hop.wait_send()

            sends.append(None)

        def share_states():
            states[y] = rows_out[0:2]
            for d in (1, 3, 2):
                send(
                    rows_out.at[0:2], states.at[y], state_sem.at[d], (z, x, 0, turn(y, d))
                )
            for d in (0, 1, 3, 2):
                send(
                    rows_out.at[2:4], states.at[y], state_sem.at[d], (z, x, 1, turn(y, d))
                )

        def pull():
            for d in (1, 3, 2) if forward else (0, 1, 3, 2):
                i = back(y, d)
                arrive(states.at[i], state_sem.at[d], (z, x, 0, i))
            loads[6].wait()
            first = 2 - 2 * c
            for l in range(2):
                block = pull_map[l]
                stage[first + 1 - l] = row_dot(
                    [(cut(block, k), states[k, l]) for k in range(B)]
                )
            share_drives(1, first)
            for l in range(2):
                filtered_out[l : l + 1] = states[y, l]

        def drive():
            loads[4].wait()
            loads[5].wait()
            for l in range(2):
                stage[2 * c + l] = row_dot([(gain[l], seen[l : l + 1])])
            share_drives(0, 2 * c)

        if forward:
            send_own()
            drive()
            compose()
            share_columns()
            finish_prefixes()
            forward_columns()
            await_drives()
            column_offsets()
            await_columns()
            pl.semaphore_signal(gate_sem, inc=1, device_id=(z, x, 1, y), device_id_type=MESH)
            send_help()
            await_shifts()
            chain(prior)
            share_states()
            pull()
            arrive(smoothed_in, smoothed_sem, (z, x, 1, y))
            for l in range(2):
                smoothed_out[l : l + 1] = smoothed_in[1 - l]
        else:
            send_help()
            drive()
            pl.semaphore_wait(gate_sem, 1)
            send_own()
            compose()
            share_columns()
            finish_prefixes()
            forward_columns()
            pull()
            await_drives()
            column_offsets()
            await_columns()
            await_shifts()
            chain(after)
            send(rows_out.at[2:4], smoothed_in, smoothed_sem, (z, x, 0, y))
            for l in range(2):
                smoothed_out[l : l + 1] = rows_out[1 - l]
        for copy in sends:
            if copy is not None:
                copy.wait_send()

    @pl.when(core == 0)
    def _():
        branch(0)

    @pl.when(core == 1)
    def _():
        branch(1)


def shards(prior_mean, after_mean, filter_map, smoother_gain, smoother_map, obs_gain, observations):
    f32 = jnp.float32
    n = B * R
    vmem = pl.BlockSpec(memory_space=pltpu.VMEM)
    hbm = pl.BlockSpec(memory_space=pl.ANY)
    dma = pltpu.SemaphoreType.DMA
    shapes = [
        (3, n, n), (R, n), (2, R, n), (2, R, n), (2, R, R), (3, R, n),
        (4, B, R, R), (4, B, B, R, R), (4, B, R, R), (2, B, R, R),
        (4, B, 1, R), (4, 1, R), (B, 4, 1, R), (4, 1, R),
        (B, 1, R), (B, 1, R), (B, 1, R), (4, 1, R), (B, 2, 1, R), (2, 1, R), (2, R),
    ]
    return pl.pallas_call(
        kernel,
        out_shape=(jax.ShapeDtypeStruct((2, R), f32), jax.ShapeDtypeStruct((2, R), f32)),
        in_specs=[vmem, vmem, hbm, hbm, hbm, hbm, hbm],
        out_specs=(vmem, vmem),
        scratch_shapes=[pltpu.VMEM(shape, f32) for shape in shapes]
        + [
            dma((7,)), dma((80,)), dma((3, B)), dma, dma((2, B)), dma((B, B, 2)),
            dma((B,)), dma((B,)), dma, dma((B,)), dma, pltpu.SemaphoreType.REGULAR,
        ],
        compiler_params=pltpu.CompilerParams(
            collective_id=0, has_side_effects=True, vmem_limit_bytes=40 * 2**20
        ),
        name="smoother",
    )(
        prior_mean.reshape(B, 1, R),
        after_mean.reshape(B, 1, R),
        filter_map,
        smoother_gain,
        smoother_map,
        obs_gain,
        observations,
    )


def solution(mesh):
    torus = Mesh(mesh.devices.reshape(8, 4, 2, mesh.shape["blk"]), (*TM, "blk"))
    in_specs = (
        P(),
        P(),
        P(TM, "blk", None),
        P(TM, "blk", None),
        P(TM, "blk", None),
        P(TM, "blk", None),
        P(TM, None),
    )
    out_specs = (P(TM, "blk"), P(TM, "blk"))
    return jax.shard_map(
        shards, mesh=torus, in_specs=in_specs, out_specs=out_specs, check_vma=False
    )
```

```python
import functools

import jax
import jax.numpy as jnp
from jax import lax
from jax.experimental import pallas as pl
from jax.experimental.pallas import tpu as pltpu
from jax.sharding import Mesh
from jax.sharding import PartitionSpec as P

TM = ("tm_0", "tm_1", "tm_2")
MESH = pl.DeviceIdType.MESH
R = 128
B = 4
Z = 8
SIDES = (1, 3)
YX, XY = (0, 2), (2, 4)
YX_PART, XY_PART = {1: (0, 1), 3: (1, 2)}, {1: (2, 3), 3: (3, 4)}
VMEM_LIMIT = 67_043_328
HIGHEST = lax.Precision.HIGHEST


def mat(a, b):
    return jnp.dot(a, b, precision=HIGHEST, preferred_element_type=jnp.float32)


def spread(row):
    return jnp.broadcast_to(row, (R, R)).T


def row_dot(pairs):
    total = None
    for a, u in pairs:
        total = a * u if total is None else total + a * u
    return jnp.sum(total.T, axis=0, keepdims=True)


def fold(product):
    return jnp.sum(product.reshape(R // 8, 8, R), axis=0)


def cut(block, k):
    return block[:, k * R : (k + 1) * R]


def kernel(
    prior,
    after,
    filter_map,
    smoother_gain,
    smoother_map,
    obs_gain,
    observations,
    both_out,
    full,
    last,
    help_rows,
    pull_map,
    gain,
    tails,
    prefix,
    columns,
    spreads,
    shift_spread,
    shifts,
    stage,
    drives,
    offsets,
    entering,
    middle,
    leaving,
    rows_out,
    states,
    smoothed_in,
    seen,
    start,
    load_sem,
    send_sem,
    full_sem,
    last_sem,
    drive_sem,
    column_sem,
    shift_y_sem,
    shift_x_sem,
    hop_sem,
    state_sem,
    smoothed_sem,
    gate_sem,
):
    filtered_out, smoothed_out = both_out.at[0], both_out.at[1]
    z, x, y = lax.axis_index("tm_0"), lax.axis_index("tm_1"), lax.axis_index("blk")
    core = lax.axis_index("tm_2")

    def branch(c):
        forward = c == 0
        own = filter_map if forward else smoother_gain
        other = smoother_gain if forward else filter_map
        place = x if forward else B - 1 - x
        level = z if forward else Z - 1 - z
        sends = []

        def x_at(p):
            return p if forward else B - 1 - p

        def turn(i, d):
            return lax.rem(i + d, B)

        def back(i, d):
            return lax.rem(i + B - d, B)

        def rows(i):
            return pl.ds(pl.multiple_of(i * R, R), R)

        def remote(src, dst, recv, device):
            return pltpu.make_async_remote_copy(
                src_ref=src,
                dst_ref=dst,
                send_sem=send_sem.at[len(sends)],
                recv_sem=recv,
                device_id=device,
                device_id_type=MESH,
            )

        def send(src, dst, recv, device):
            copy = remote(src, dst, recv, device)
            copy.start()
            sends.append(copy)

        def arrive(dst, recv, device):
            pltpu.make_async_remote_copy(
                src_ref=dst,
                dst_ref=dst,
                send_sem=send_sem.at[0],
                recv_sem=recv,
                device_id=device,
                device_id_type=MESH,
            ).wait_recv()

        loads = []

        def load(src, dst):
            copy = pltpu.make_async_copy(src, dst, load_sem.at[len(loads)])
            copy.start()
            loads.append(copy)

        load(own.at[c], full.at[0, rows(y)])
        load(own.at[1 - c], full.at[1, rows(y)])
        load(other.at[1 - c], help_rows.at[0])
        load(other.at[c], help_rows.at[1])
        load(obs_gain, gain)
        load(observations, seen)
        load(smoother_map, pull_map)
        load(prior if forward else after, start)

        barrier = pltpu.get_barrier_semaphore()
        peers = [(z, x, c, turn(y, d)) for d in (1, 2, 3)]
        peers += [(z, x, 1 - c, turn(y, d)) for d in (0, 1, 2, 3)]
        peers += [(z, turn(x, d), c, y) for d in (1, 2, 3)]
        peers += [(lax.rem(z + 1, Z), x, c, y), (lax.rem(z + Z - 1, Z), x, c, y)]
        for peer in peers:
            pl.semaphore_signal(barrier, inc=1, device_id=peer, device_id_type=MESH)
        pl.semaphore_wait(barrier, len(peers))

        def block(n, i, h=None):
            if h is None:
                return full.at[n, rows(i)]
            return full.at[n, pl.ds(pl.multiple_of(i * R + h * (R // 2), R // 2), R // 2)]

        def send_own():
            for n in (1, 0):
                loads[n].wait()
                for d in (1, 3):
                    mine = block(n, y)
                    send(mine, mine, full_sem.at[n, d, 0], (z, x, c, turn(y, d)))

        def send_help():
            loads[2].wait()
            for d in (1, 3, 0):
                send(
                    help_rows.at[0],
                    block(2, y),
                    full_sem.at[2, d, 0],
                    (z, x, 1 - c, turn(y, d)),
                )
            loads[3].wait()
            send(help_rows.at[1], last, last_sem, (z, x, 1 - c, y))

        def pass_on(n):
            for d, h in ((1, 0), (3, 1)):
                i = back(y, d)
                arrive(block(n, i), full_sem.at[n, d, 0], (z, x, c, i))
                mine = block(n, i, h)
                send(mine, mine, full_sem.at[n, 2, h], (z, x, c, turn(y, d)))

        def await_far(n):
            for h in (0, 1):
                i = back(y, 2)
                arrive(block(n, i, h), full_sem.at[n, 2, h], (z, x, c, i))

        def share_drives(to, first):
            if to == c:
                drives[y, first : first + 2] = stage[first : first + 2]
            for d in (1, 3, 2) if to == c else (0, 1, 3, 2):
                send(
                    stage.at[first : first + 2],
                    drives.at[y, first : first + 2],
                    drive_sem.at[c, d],
                    (z, x, to, turn(y, d)),
                )

        def await_drives():
            for cc in (c, 1 - c):
                first = 2 * cc if forward else 2 - 2 * cc
                for d in (1, 3, 2) if cc == c else (0, 1, 3, 2):
                    i = back(y, d)
                    arrive(
                        drives.at[i, first : first + 2], drive_sem.at[cc, d], (z, x, cc, i)
                    )

        def compose():
            for n in (2, 1, 0):
                pass_on(n)
            arrive(block(2, y), full_sem.at[2, 0, 0], (z, x, 1 - c, y))
            arrive(last, last_sem, (z, x, 1 - c, y))
            await_far(2)
            tails[0] = mat(last[...], full[2])
            await_far(1)
            tails[1] = mat(tails[0], full[1])
            if forward:
                await_drives()
                share_shift()
            await_far(0)
            whole = mat(tails[1], full[0])
            turned = [cut(whole, k).T for k in range(B)]
            for k in range(B):
                prefix[3, k] = turned[k]

            @pl.when(lax.rem(place, 2) == 0)
            def _():
                for k in range(B):
                    columns[place, y, k] = cut(whole, k)

            @pl.when(lax.rem(place, 2) == 1)
            def _():
                for k in range(B):
                    columns[place, y, k] = turned[k]

        def piece(dp, d, k):
            return columns.at[back(place, dp), back(y, d), k[0] : k[1]]

        def to_y(dp, d, k, e):
            mine = piece(dp, d, k)
            send(mine, mine, column_sem.at[dp, (d + e) % B, k[0]], (z, x, c, turn(y, e)))

        def to_x(dp, d, k, e):
            mine = piece(dp, d, k)
            device = (z, x_at(turn(place, e)), c, y)
            send(mine, mine, column_sem.at[(dp + e) % B, d, k[0]], device)

        def got(dp, d, k):
            arrive(piece(dp, d, k), column_sem.at[dp, d, k[0]], (z, x, c, back(y, 1)))

        def share_columns():
            for to, k in ((to_y, YX), (to_x, XY), (to_x, YX), (to_y, XY)):
                for e in SIDES:
                    to(0, 0, k, e)

        def finish_prefixes():
            mine = full[1, rows(y)]
            tails[2] = mat(full[2, rows(y)], full[1])
            first = mat(mine, full[0])
            second = mat(tails[2], full[0])
            zeroth = full[0, rows(y)]
            for k in range(B):
                prefix[0, k] = cut(zeroth, k).T
                prefix[1, k] = cut(first, k).T
                prefix[2, k] = cut(second, k).T

        def relay(d):
            for e in SIDES:
                got(e, d, YX)
                to_x(e, d, YX_PART[e], e)
                got(d, e, XY)
                to_y(d, e, XY_PART[e], e)

        def forward_columns():
            for e in SIDES:
                got(0, e, YX)
                to_y(0, e, YX_PART[e], e)
                got(e, 0, XY)
                to_x(e, 0, XY_PART[e], e)
            if forward:
                spread_shift()
            for d in SIDES:
                for e in SIDES:
                    to_x(0, d, YX, e)
                    to_y(d, 0, XY, e)
            relay(0)
            for e in SIDES:
                got(0, 2, YX_PART[e])
                got(2, 0, XY_PART[e])
            for e in SIDES:
                to_x(0, 2, YX, e)
                to_y(2, 0, XY, e)
            for d in (1, 3, 2):
                relay(d)

        def await_columns():
            for d in range(B):
                for e in SIDES:
                    got(2, d, YX_PART[e])
                    got(d, 2, XY_PART[e])

        def pairs(rows_of_map, i):
            return [(cut(rows_of_map, k), drives[k, i]) for k in range(B)]

        def share_shift():
            parts = pairs(tails[1], 0) + pairs(tails[0], 1) + pairs(last[...], 2)
            shift = row_dot(parts) + drives[y, 3]
            offsets[3] = shift
            shifts[place, y] = shift
            mine = shifts.at[place, y]
            for e in (1, 3, 2):
                send(mine, mine, shift_y_sem.at[e], (z, x, c, turn(y, e)))

        def spread_shift():
            for e in (1, 3, 2):
                i = back(y, e)
                arrive(shifts.at[place, i], shift_y_sem.at[e], (z, x, c, i))
            mine = shifts.at[place]
            for e in (1, 3, 2):
                send(mine, mine, shift_x_sem.at[e], (z, x_at(turn(place, e)), c, y))

        def other_offsets():
            third = row_dot(pairs(tails[2], 0) + pairs(full[2, rows(y)], 1))
            offsets[2] = third + drives[y, 2]
            offsets[1] = row_dot(pairs(full[1, rows(y)], 0)) + drives[y, 1]
            offsets[0] = drives[y, 0]

        def await_shifts():
            for e in (1, 3, 2):
                p = back(place, e)
                arrive(shifts.at[p], shift_x_sem.at[e], (z, x_at(p), c, y))
            for n in range(2):
                for k in range(B):
                    shift_spread[n, k] = spread(shifts[2 * n, k])

        def pair(n, state):
            for i in range(B):
                total = None
                for k in range(B):
                    term = columns[2 * n, i, k] * state[k]
                    total = term if total is None else total + term
                reduced = jnp.sum(total, axis=1, keepdims=True)
                spreads[2 * n + 1, i] = jnp.broadcast_to(reduced, (R, R)) + shift_spread[n, i]
            result = []
            for i in range(B):
                total = None
                for k in range(B):
                    term = fold(columns[2 * n + 1, i, k] * spreads[2 * n + 1, k])
                    total = term if total is None else total + term
                result.append(jnp.sum(total, axis=0, keepdims=True) + shifts[2 * n + 1, i])
            return result

        def chain():
            up, down = (z + 1, z - 1) if forward else (z - 1, z + 1)

            @pl.when(level == 0)
            def _():
                entering[...] = start[...]

            @pl.when(level > 0)
            def _():
                arrive(entering, hop_sem, (down, x, c, y))

            state = pair(0, [entering[k] for k in range(B)])
            for k in range(B):
                middle[k] = state[k]
            state = pair(1, state)
            for k in range(B):
                leaving[k] = state[k]
            hop = remote(leaving, entering, hop_sem, (up, x, c, y))

            @pl.when(level < Z - 1)
            def _():
                hop.start()

            @pl.when(place == 0)
            def _():
                for k in range(B):
                    spreads[0, k] = spread(entering[k])

            @pl.when(place == 2)
            def _():
                for k in range(B):
                    spreads[2, k] = spread(middle[k])

            for i in range(4):
                total = None
                for k in range(B):
                    term = fold(prefix[i, k] * spreads[place, k])
                    total = term if total is None else total + term
                rows_out[i] = jnp.sum(total, axis=0, keepdims=True) + offsets[i]

            @pl.when(level < Z - 1)
            def _():
                hop.wait_send()

            sends.append(None)

        def share_states():
            states[y] = rows_out[0:2]
            for d in (1, 3, 2):
                send(
                    rows_out.at[0:2], states.at[y], state_sem.at[d], (z, x, 0, turn(y, d))
                )
            for d in (0, 1, 3, 2):
                send(
                    rows_out.at[2:4], states.at[y], state_sem.at[d], (z, x, 1, turn(y, d))
                )

        def pull():
            for d in (1, 3, 2) if forward else (0, 1, 3, 2):
                i = back(y, d)
                arrive(states.at[i], state_sem.at[d], (z, x, 0, i))
            loads[6].wait()
            first = 2 - 2 * c
            for l in range(2):
                block = pull_map[l]
                stage[first + 1 - l] = row_dot(
                    [(cut(block, k), states[k, l]) for k in range(B)]
                )
            share_drives(1, first)
            for l in range(2):
                filtered_out[l : l + 1] = states[y, l]

        def drive():
            loads[4].wait()
            loads[5].wait()
            for l in range(2):
                stage[2 * c + l] = row_dot([(gain[l], seen[l : l + 1])])
            share_drives(0, 2 * c)

        if forward:
            send_own()
            drive()
            compose()
            share_columns()
            finish_prefixes()
            forward_columns()
            pl.semaphore_signal(gate_sem, inc=1, device_id=(z, x, 1, y), device_id_type=MESH)
            send_help()
            other_offsets()
            await_shifts()
            await_columns()
            loads[7].wait()
            chain()
            share_states()
            pull()
            arrive(smoothed_in, smoothed_sem, (z, x, 1, y))
            for l in range(2):
                smoothed_out[l : l + 1] = smoothed_in[1 - l]
        else:
            send_help()
            drive()
            pl.semaphore_wait(gate_sem, 1)
            send_own()
            compose()
            share_columns()
            finish_prefixes()
            forward_columns()
            pull()
            await_drives()
            share_shift()
            spread_shift()
            other_offsets()
            await_shifts()
            await_columns()
            loads[7].wait()
            chain()
            send(rows_out.at[2:4], smoothed_in, smoothed_sem, (z, x, 0, y))
            for l in range(2):
                smoothed_out[l : l + 1] = rows_out[1 - l]
        for copy in sends:
            if copy is not None:
                copy.wait_send()

    @pl.when(core == 0)
    def _():
        branch(0)

    @pl.when(core == 1)
    def _():
        branch(1)


def shards(prior_mean, after_mean, filter_map, smoother_gain, smoother_map, obs_gain, observations):
    f32 = jnp.float32
    n = B * R
    vmem = pl.BlockSpec(memory_space=pltpu.VMEM)
    hbm = pl.BlockSpec(memory_space=pltpu.HBM)
    dma = pltpu.SemaphoreType.DMA
    shapes = [
        (3, n, n), (R, n), (2, R, n), (2, R, n), (2, R, R), (3, R, n),
        (4, B, R, R), (4, B, B, R, R), (4, B, R, R), (2, B, R, R),
        (4, B, 1, R), (4, 1, R), (B, 4, 1, R), (4, 1, R),
        (B, 1, R), (B, 1, R), (B, 1, R), (4, 1, R), (B, 2, 1, R), (2, 1, R), (2, R), (B, 1, R),
    ]
    both = pl.pallas_call(
        kernel,
        out_shape=jax.ShapeDtypeStruct((2, 2, R), f32),
        in_specs=[hbm] * 7,
        out_specs=vmem,
        scratch_shapes=[pltpu.VMEM(shape, f32) for shape in shapes]
        + [
            dma((8,)), dma((96,)), dma((3, B, 2)), dma, dma((2, B)), dma((B, B, 4)),
            dma((B,)), dma((B,)), dma, dma((B,)), dma, pltpu.SemaphoreType.REGULAR,
        ],
        compiler_params=pltpu.CompilerParams(
            collective_id=0, has_side_effects=True, vmem_limit_bytes=VMEM_LIMIT
        ),
        name="smoother",
    )(
        prior_mean.reshape(B, 1, R),
        after_mean.reshape(B, 1, R),
        filter_map,
        smoother_gain,
        smoother_map,
        obs_gain,
        observations,
    )
    return both[0], both[1]


def solution(mesh):
    torus = Mesh(mesh.devices.reshape(8, 4, 2, mesh.shape["blk"]), (*TM, "blk"))
    in_specs = (
        P(),
        P(),
        P(TM, "blk", None),
        P(TM, "blk", None),
        P(TM, "blk", None),
        P(TM, "blk", None),
        P(TM, None),
    )
    out_specs = (P(TM, "blk"), P(TM, "blk"))
    return jax.shard_map(
        shards, mesh=torus, in_specs=in_specs, out_specs=out_specs, check_vma=False
    )
```

```python
import functools

import jax
import jax.numpy as jnp
from jax import lax
from jax.experimental import pallas as pl
from jax.experimental.pallas import tpu as pltpu
from jax.sharding import Mesh
from jax.sharding import PartitionSpec as P

TM = ("tm_0", "tm_1", "tm_2")
MESH = pl.DeviceIdType.MESH
R = 128
B = 4
Z = 8
GATE = 3
SIDES = (1, 3)
YX, XY = (0, 2), (2, 4)
YX_PART, XY_PART = {1: (0, 1), 3: (1, 2)}, {1: (2, 3), 3: (3, 4)}
VMEM_LIMIT = 67_043_328


def mat(a, b):
    high, low = [], []
    for value in (a, b):
        top = value.astype(jnp.bfloat16)
        high.append(top)
        low.append((value - top.astype(jnp.float32)).astype(jnp.bfloat16))
    dot = functools.partial(jnp.dot, preferred_element_type=jnp.float32)
    return dot(high[0], high[1]) + (dot(high[0], low[1]) + dot(low[0], high[1]))


def spread(row):
    return jnp.broadcast_to(row, (R, R)).T


def row_dot(pairs):
    total = None
    for a, u in pairs:
        total = a * u if total is None else total + a * u
    return jnp.sum(total.T, axis=0, keepdims=True)


def fold(product):
    return jnp.sum(product.reshape(R // 8, 8, R), axis=0)


def cut(block, k):
    return block[:, k * R : (k + 1) * R]


def kernel(
    prior,
    after,
    filter_map,
    smoother_gain,
    smoother_map,
    obs_gain,
    observations,
    both_out,
    full,
    last,
    help_rows,
    pull_map,
    gain,
    tails,
    prefix,
    columns,
    spreads,
    shift_spread,
    shifts,
    stage,
    drives,
    offsets,
    entering,
    middle,
    leaving,
    rows_out,
    states,
    smoothed_in,
    seen,
    start,
    back_tails,
    pulled,
    back_shift,
    filtered_in,
    load_sem,
    send_sem,
    full_sem,
    last_sem,
    drive_sem,
    column_sem,
    shift_y_sem,
    shift_x_sem,
    hop_sem,
    state_sem,
    smoothed_sem,
    gate_sem,
    pull_sem,
    tails_sem,
    pulled_sem,
    drives_sem,
    back_shift_sem,
    filtered_sem,
):
    filtered_out, smoothed_out = both_out.at[0], both_out.at[1]
    z, x, y = lax.axis_index("tm_0"), lax.axis_index("tm_1"), lax.axis_index("blk")
    core = lax.axis_index("tm_2")

    def branch(c):
        forward = c == 0
        own = filter_map if forward else smoother_gain
        other = smoother_gain if forward else filter_map
        place = x if forward else B - 1 - x
        level = z if forward else Z - 1 - z
        sends = []

        def x_at(p):
            return p if forward else B - 1 - p

        def turn(i, d):
            return lax.rem(i + d, B)

        def back(i, d):
            return lax.rem(i + B - d, B)

        def rows(i):
            return pl.ds(pl.multiple_of(i * R, R), R)

        def remote(src, dst, recv, device):
            return pltpu.make_async_remote_copy(
                src_ref=src,
                dst_ref=dst,
                send_sem=send_sem.at[len(sends)],
                recv_sem=recv,
                device_id=device,
                device_id_type=MESH,
            )

        def send(src, dst, recv, device):
            copy = remote(src, dst, recv, device)
            copy.start()
            sends.append(copy)

        def arrive(dst, recv, device):
            pltpu.make_async_remote_copy(
                src_ref=dst,
                dst_ref=dst,
                send_sem=send_sem.at[0],
                recv_sem=recv,
                device_id=device,
                device_id_type=MESH,
            ).wait_recv()

        loads = []

        def load(src, dst):
            copy = pltpu.make_async_copy(src, dst, load_sem.at[len(loads)])
            copy.start()
            loads.append(copy)

        load(own.at[c], full.at[0, rows(y)])
        load(own.at[1 - c], full.at[1, rows(y)])
        load(other.at[1 - c], help_rows.at[0])
        load(other.at[c], help_rows.at[1])
        load(obs_gain, gain)
        load(observations, seen)
        load(smoother_map, pull_map.at[2 * c : 2 * c + 2])
        load(prior if forward else after, start)

        barrier = pltpu.get_barrier_semaphore()
        peers = [(z, x, c, turn(y, d)) for d in (1, 2, 3)]
        peers += [(z, turn(x, d), c, y) for d in (1, 2, 3)]
        peers += [(lax.rem(z + 1, Z), x, c, y), (lax.rem(z + Z - 1, Z), x, c, y)]
        peers += [(z, turn(x, e), 1 - c, turn(y, d)) for e in range(B) for d in range(B)]
        for peer in peers:
            pl.semaphore_signal(barrier, inc=1, device_id=peer, device_id_type=MESH)
        pl.semaphore_wait(barrier, len(peers))

        def block(n, i, h=None):
            if h is None:
                return full.at[n, rows(i)]
            return full.at[n, pl.ds(pl.multiple_of(i * R + h * (R // 2), R // 2), R // 2)]

        def send_own():
            for n in (1, 0):
                loads[n].wait()
                for d in SIDES:
                    mine = block(n, y)
                    send(mine, mine, full_sem.at[n, d, 0], (z, x, c, turn(y, d)))

        def send_help():
            loads[2].wait()
            for d in (1, 3, 0):
                device = (z, x, 1 - c, turn(y, d))
                send(help_rows.at[0], block(2, y), full_sem.at[2, d, 0], device)
            loads[3].wait()
            send(help_rows.at[1], last, last_sem, (z, x, 1 - c, y))

        def pass_on(n):
            for d, h in ((1, 0), (3, 1)):
                i = back(y, d)
                arrive(block(n, i), full_sem.at[n, d, 0], (z, x, c, i))
                mine = block(n, i, h)
                send(mine, mine, full_sem.at[n, 2, h], (z, x, c, turn(y, d)))

        def await_far(n):
            for h in (0, 1):
                i = back(y, 2)
                arrive(block(n, i, h), full_sem.at[n, 2, h], (z, x, c, i))

        def drive():
            loads[4].wait()
            loads[5].wait()
            first = 2 * c
            for l in range(2):
                stage[first + l] = row_dot([(gain[l], seen[l : l + 1])])
            mine = stage.at[first : first + 2]
            if forward:
                drives[y, 0:2] = stage[0:2]
            for d in (1, 3, 2) if forward else (0, 1, 3, 2):
                target = drives.at[y, first : first + 2]
                send(mine, target, drive_sem.at[c, d], (z, x, 0, turn(y, d)))

        def await_drives():
            for cc in (0, 1):
                for d in (1, 3, 2) if cc == 0 else (0, 1, 3, 2):
                    i = back(y, d)
                    target = drives.at[i, 2 * cc : 2 * cc + 2]
                    arrive(target, drive_sem.at[cc, d], (z, x, cc, i))

        def compose():
            for n in (2, 1, 0):
                pass_on(n)
            if forward:
                send_help()
            arrive(block(2, y), full_sem.at[2, 0, 0], (z, x, 1 - c, y))
            arrive(last, last_sem, (z, x, 1 - c, y))
            await_far(2)
            tails[0] = mat(last[...], full[2])
            await_far(1)
            tails[1] = mat(tails[0], full[1])
            if forward:
                await_drives()
                share_shift()
            await_far(0)
            whole = mat(tails[1], full[0])
            turned = [cut(whole, k).T for k in range(B)]
            for k in range(B):
                prefix[3, k] = turned[k]

            @pl.when(lax.rem(place, 2) == 0)
            def _():
                for k in range(B):
                    columns[place, y, k] = cut(whole, k)

            @pl.when(lax.rem(place, 2) == 1)
            def _():
                for k in range(B):
                    columns[place, y, k] = turned[k]

        def piece(dp, d, k):
            return columns.at[back(place, dp), back(y, d), k[0] : k[1]]

        def to_y(dp, d, k, e):
            mine = piece(dp, d, k)
            send(mine, mine, column_sem.at[dp, (d + e) % B, k[0]], (z, x, c, turn(y, e)))

        def to_x(dp, d, k, e):
            mine = piece(dp, d, k)
            device = (z, x_at(turn(place, e)), c, y)
            send(mine, mine, column_sem.at[(dp + e) % B, d, k[0]], device)

        def got(dp, d, k):
            arrive(piece(dp, d, k), column_sem.at[dp, d, k[0]], (z, x, c, back(y, 1)))

        def share_columns():
            for to, k in ((to_y, YX), (to_x, XY), (to_x, YX), (to_y, XY)):
                for e in SIDES:
                    to(0, 0, k, e)

        def finish_prefixes():
            tails[2] = mat(full[2, rows(y)], full[1])
            both = mat(jnp.concatenate([full[1, rows(y)], tails[2]], axis=0), full[0])
            first, second = both[:R], both[R:]
            zeroth = full[0, rows(y)]
            for k in range(B):
                prefix[0, k] = cut(zeroth, k).T
                prefix[1, k] = cut(first, k).T
                prefix[2, k] = cut(second, k).T

        def relay(d):
            for e in SIDES:
                got(e, d, YX)
                to_x(e, d, YX_PART[e], e)
                got(d, e, XY)
                to_y(d, e, XY_PART[e], e)

        def forward_columns():
            for e in SIDES:
                got(0, e, YX)
                to_y(0, e, YX_PART[e], e)
                got(e, 0, XY)
                to_x(e, 0, XY_PART[e], e)
            if forward:
                spread_shift()
            for d in SIDES:
                for e in SIDES:
                    to_x(0, d, YX, e)
                    to_y(d, 0, XY, e)
            if forward:
                open_gate(2)
            relay(0)
            for e in SIDES:
                got(0, 2, YX_PART[e])
                got(2, 0, XY_PART[e])
            for e in (1, 3, 2):
                to_x(0, 2, YX, e)
                to_y(2, 0, XY, e)
            for d in (1, 3):
                relay(d)
            for e in SIDES:
                got(e, 2, YX)
                got(2, e, XY)

        def await_columns():
            for d in (0, 1, 3):
                for e in SIDES:
                    got(2, d, YX_PART[e])
                    got(d, 2, XY_PART[e])
            got(2, 2, YX)
            got(2, 2, XY)

        def pairs(rows_of_map, i):
            return [(cut(rows_of_map, k), drives[k, i]) for k in range(B)]

        def share_shift():
            parts = pairs(tails[1], 0) + pairs(tails[0], 1) + pairs(last[...], 2)
            shift = row_dot(parts) + drives[y, 3]
            offsets[3] = shift
            shifts[place, y] = shift
            mine = shifts.at[place, y]
            for e in (1, 3, 2):
                send(mine, mine, shift_y_sem.at[e], (z, x, c, turn(y, e)))

        def spread_shift():
            for e in (1, 3, 2):
                i = back(y, e)
                arrive(shifts.at[place, i], shift_y_sem.at[e], (z, x, c, i))
            mine = shifts.at[place]
            for e in (1, 3, 2):
                send(mine, mine, shift_x_sem.at[e], (z, x_at(turn(place, e)), c, y))

        def other_offsets():
            third = row_dot(pairs(tails[2], 0) + pairs(full[2, rows(y)], 1))
            offsets[2] = third + drives[y, 2]
            offsets[1] = row_dot(pairs(full[1, rows(y)], 0)) + drives[y, 1]
            offsets[0] = drives[y, 0]

        def await_shifts():
            if forward:
                for e in (1, 3, 2):
                    p = back(place, e)
                    arrive(shifts.at[p], shift_x_sem.at[e], (z, x_at(p), c, y))
            else:
                for e in range(B):
                    p = back(place, e)
                    for d in range(B):
                        i = back(y, d)
                        arrive(shifts.at[p, i], back_shift_sem.at[e, d], (z, x_at(p), 0, i))
            for n in range(2):
                for k in range(B):
                    shift_spread[n, k] = spread(shifts[2 * n, k])

        def pair(n, state):
            for i in range(B):
                total = None
                for k in range(B):
                    term = columns[2 * n, i, k] * state[k]
                    total = term if total is None else total + term
                reduced = jnp.sum(total, axis=1, keepdims=True)
                spreads[2 * n + 1, i] = jnp.broadcast_to(reduced, (R, R)) + shift_spread[n, i]
            result = []
            for i in range(B):
                total = None
                for k in range(B):
                    term = fold(columns[2 * n + 1, i, k] * spreads[2 * n + 1, k])
                    total = term if total is None else total + term
                result.append(jnp.sum(total, axis=0, keepdims=True) + shifts[2 * n + 1, i])
            return result

        def open_gate(n):
            if n == GATE:
                pl.semaphore_signal(
                    gate_sem, inc=1, device_id=(z, x, 1, y), device_id_type=MESH
                )

        def back_offsets():
            arrive(drives, drives_sem, (z, x, 0, y))
            other_offsets()
            offsets[3] = shifts[place, y]

        def chain():
            up, down = (z + 1, z - 1) if forward else (z - 1, z + 1)

            @pl.when(level == 0)
            def _():
                entering[...] = start[...]

            @pl.when(level > 0)
            def _():
                if not forward:
                    back_offsets()
                arrive(entering, hop_sem, (down, x, c, y))

            state = pair(0, [entering[k] for k in range(B)])
            for k in range(B):
                middle[k] = state[k]
            state = pair(1, state)
            for k in range(B):
                leaving[k] = state[k]
            hop = remote(leaving, entering, hop_sem, (up, x, c, y))

            @pl.when(level < Z - 1)
            def _():
                hop.start()

            @pl.when(place == 0)
            def _():
                for k in range(B):
                    spreads[0, k] = spread(entering[k])

            @pl.when(place == 2)
            def _():
                for k in range(B):
                    spreads[2, k] = spread(middle[k])

            if not forward:

                @pl.when(level == 0)
                def _():
                    back_offsets()

            for i in range(4):
                total = None
                for k in range(B):
                    term = fold(prefix[i, k] * spreads[place, k])
                    total = term if total is None else total + term
                rows_out[i] = jnp.sum(total, axis=0, keepdims=True) + offsets[i]

            @pl.when(level < Z - 1)
            def _():
                hop.wait_send()

            sends.append(None)

        def share_states():
            states[y] = rows_out[...]
            for d in (1, 3, 2):
                send(rows_out, states.at[y], state_sem.at[d], (z, x, 0, turn(y, d)))
            send(rows_out.at[2:4], filtered_in, filtered_sem, (z, x, 1, y))
            for d in (1, 3, 2):
                i = back(y, d)
                arrive(states.at[i], state_sem.at[d], (z, x, 0, i))

        def pull():
            loads[6].wait()
            arrive(pull_map.at[2:4], pull_sem, (z, x, 1, y))
            for i in range(4):
                step = pull_map[3 - i]
                pulled[y, i] = row_dot([(cut(step, k), states[k, 3 - i]) for k in range(B)])
            mine = pulled.at[y]
            for d in (1, 3, 2):
                send(mine, mine, pulled_sem.at[d], (z, x, 0, turn(y, d)))
            arrive(back_tails, tails_sem, (z, x, 1, y))
            for d in (1, 3, 2):
                i = back(y, d)
                arrive(pulled.at[i], pulled_sem.at[d], (z, x, 0, i))
            maps = (back_tails[1], back_tails[0], help_rows[1])
            parts = [(cut(a, k), pulled[k, i]) for i, a in enumerate(maps) for k in range(B)]
            back_shift[...] = row_dot(parts) + pulled[y, 3]
            p = B - 1 - x
            for e in range(B):
                for d in range(B):
                    device = (z, B - 1 - turn(p, e), 1, turn(y, d))
                    send(back_shift, shifts.at[p, y], back_shift_sem.at[e, d], device)
            send(pulled, drives, drives_sem, (z, x, 1, y))

        if forward:
            send_own()
            drive()
            compose()
            open_gate(0)
            share_columns()
            open_gate(1)
            finish_prefixes()
            forward_columns()
            open_gate(3)
            other_offsets()
            await_shifts()
            await_columns()
            loads[7].wait()
            chain()
            share_states()
            pull()
            for l in range(2):
                filtered_out[l : l + 1] = rows_out[l]
            arrive(smoothed_in, smoothed_sem, (z, x, 1, y))
            for l in range(2):
                smoothed_out[l : l + 1] = smoothed_in[1 - l]
        else:
            send_help()
            drive()
            loads[6].wait()
            send(pull_map.at[2:4], pull_map.at[2:4], pull_sem, (z, x, 0, y))
            pl.semaphore_wait(gate_sem, 1)
            send_own()
            compose()
            send(tails.at[0:2], back_tails, tails_sem, (z, x, 0, y))
            share_columns()
            finish_prefixes()
            forward_columns()
            await_shifts()
            await_columns()
            loads[7].wait()
            chain()
            send(rows_out.at[2:4], smoothed_in, smoothed_sem, (z, x, 0, y))
            arrive(filtered_in, filtered_sem, (z, x, 0, y))
            for l in range(2):
                filtered_out[l : l + 1] = filtered_in[l]
                smoothed_out[l : l + 1] = rows_out[1 - l]
        for copy in sends:
            if copy is not None:
                copy.wait_send()

    @pl.when(core == 0)
    def _():
        branch(0)

    @pl.when(core == 1)
    def _():
        branch(1)


def shards(prior_mean, after_mean, filter_map, smoother_gain, smoother_map, obs_gain, observations):
    f32 = jnp.float32
    n = B * R
    vmem = pl.BlockSpec(memory_space=pltpu.VMEM)
    hbm = pl.BlockSpec(memory_space=pltpu.HBM)
    dma = pltpu.SemaphoreType.DMA
    shapes = [
        (3, n, n), (R, n), (2, R, n), (4, R, n), (2, R, R), (3, R, n),
        (4, B, R, R), (4, B, B, R, R), (4, B, R, R), (2, B, R, R),
        (4, B, 1, R), (4, 1, R), (B, 4, 1, R), (4, 1, R),
        (B, 1, R), (B, 1, R), (B, 1, R), (4, 1, R), (B, 4, 1, R), (2, 1, R), (2, R), (B, 1, R),
        (2, R, n), (B, 4, 1, R), (1, R), (2, 1, R),
    ]
    both = pl.pallas_call(
        kernel,
        out_shape=jax.ShapeDtypeStruct((2, 2, R), f32),
        in_specs=[hbm] * 7,
        out_specs=vmem,
        scratch_shapes=[pltpu.VMEM(shape, f32) for shape in shapes]
        + [
            dma((8,)), dma((96,)), dma((3, B, 2)), dma, dma((2, B)), dma((B, B, 4)),
            dma((B,)), dma((B,)), dma, dma((B,)), dma, pltpu.SemaphoreType.REGULAR,
            dma, dma, dma((B,)), dma, dma((B, B)), dma,
        ],
        compiler_params=pltpu.CompilerParams(
            collective_id=0, has_side_effects=True, vmem_limit_bytes=VMEM_LIMIT
        ),
        name="smoother",
    )(
        prior_mean.reshape(B, 1, R),
        after_mean.reshape(B, 1, R),
        filter_map,
        smoother_gain,
        smoother_map,
        obs_gain,
        observations,
    )
    return both[0], both[1]


def solution(mesh):
    torus = Mesh(mesh.devices.reshape(8, 4, 2, mesh.shape["blk"]), (*TM, "blk"))
    in_specs = (
        P(),
        P(),
        P(TM, "blk", None),
        P(TM, "blk", None),
        P(TM, "blk", None),
        P(TM, "blk", None),
        P(TM, None),
    )
    out_specs = (P(TM, "blk"), P(TM, "blk"))
    return jax.shard_map(
        shards, mesh=torus, in_specs=in_specs, out_specs=out_specs, check_vma=False
    )
```

```python
import functools

import jax
import jax.numpy as jnp
from jax import lax
from jax.experimental import pallas as pl
from jax.experimental.pallas import tpu as pltpu
from jax.sharding import Mesh
from jax.sharding import PartitionSpec as P

TM = ("tm_0", "tm_1", "tm_2")
MESH = pl.DeviceIdType.MESH
R = 128
B = 4
Z = 8
SIDES = (1, 3)
YX, XY = (0, 2), (2, 4)
YX_PART, XY_PART = {1: (0, 1), 3: (1, 2)}, {1: (2, 3), 3: (3, 4)}
VMEM_LIMIT = 67_043_328


def mat(a, b):
    high, low = [], []
    for value in (a, b):
        top = value.astype(jnp.bfloat16)
        high.append(top)
        low.append((value - top.astype(jnp.float32)).astype(jnp.bfloat16))
    dot = functools.partial(jnp.dot, preferred_element_type=jnp.float32)
    return dot(high[0], high[1]) + (dot(high[0], low[1]) + dot(low[0], high[1]))


def spread(row):
    return jnp.broadcast_to(row, (R, R)).T


def row_dot(pairs):
    total = None
    for a, u in pairs:
        total = a * u if total is None else total + a * u
    return jnp.sum(total.T, axis=0, keepdims=True)


def fold(product):
    return jnp.sum(product.reshape(R // 8, 8, R), axis=0)


def cut(block, k):
    return block[:, k * R : (k + 1) * R]


def kernel(
    prior,
    after,
    filter_map,
    smoother_gain,
    smoother_map,
    obs_gain,
    observations,
    both_out,
    full,
    last,
    help_rows,
    pull_map,
    gain,
    tails,
    prefix,
    columns,
    spreads,
    shift_spread,
    shifts,
    stage,
    drives,
    offsets,
    entering,
    middle,
    leaving,
    rows_out,
    states,
    smoothed_in,
    seen,
    start,
    back_tails,
    pulled,
    back_shift,
    filtered_in,
    first,
    load_sem,
    send_sem,
    full_sem,
    last_sem,
    drive_sem,
    column_sem,
    shift_y_sem,
    shift_x_sem,
    hop_sem,
    smoothed_sem,
    gate_sem,
    pull_sem,
    tails_sem,
    pulled_sem,
    drives_sem,
    back_shift_sem,
    filtered_sem,
):
    filtered_out, smoothed_out = both_out.at[0], both_out.at[1]
    z, x, y = lax.axis_index("tm_0"), lax.axis_index("tm_1"), lax.axis_index("blk")
    core = lax.axis_index("tm_2")

    def branch(c):
        forward = c == 0
        own = filter_map if forward else smoother_gain
        other = smoother_gain if forward else filter_map
        place = x if forward else B - 1 - x
        level = z if forward else Z - 1 - z
        sends = []

        def x_at(p):
            return p if forward else B - 1 - p

        def turn(i, d):
            return lax.rem(i + d, B)

        def back(i, d):
            return lax.rem(i + B - d, B)

        def rows(i):
            return pl.ds(pl.multiple_of(i * R, R), R)

        def remote(src, dst, recv, device):
            return pltpu.make_async_remote_copy(
                src_ref=src,
                dst_ref=dst,
                send_sem=send_sem.at[len(sends)],
                recv_sem=recv,
                device_id=device,
                device_id_type=MESH,
            )

        def send(src, dst, recv, device):
            copy = remote(src, dst, recv, device)
            copy.start()
            sends.append(copy)

        def arrive(dst, recv, device):
            pltpu.make_async_remote_copy(
                src_ref=dst,
                dst_ref=dst,
                send_sem=send_sem.at[0],
                recv_sem=recv,
                device_id=device,
                device_id_type=MESH,
            ).wait_recv()

        loads = []

        def load(src, dst):
            copy = pltpu.make_async_copy(src, dst, load_sem.at[len(loads)])
            copy.start()
            loads.append(copy)

        load(own.at[c], full.at[0, rows(y)])
        load(own.at[1 - c], full.at[1, rows(y)])
        load(other.at[1 - c], help_rows.at[0])
        load(other.at[c], help_rows.at[1])
        load(obs_gain, gain)
        load(observations, seen)
        load(smoother_map, pull_map.at[2 * c : 2 * c + 2])
        load(prior if forward else after, start)

        barrier = pltpu.get_barrier_semaphore()
        peers = [(z, x, c, turn(y, d)) for d in (1, 2, 3)]
        peers += [(z, turn(x, d), c, y) for d in (1, 2, 3)]
        peers += [(lax.rem(z + 1, Z), x, c, y), (lax.rem(z + Z - 1, Z), x, c, y)]
        peers += [(z, turn(x, e), 1 - c, turn(y, d)) for e in range(B) for d in range(B)]
        for peer in peers:
            pl.semaphore_signal(barrier, inc=1, device_id=peer, device_id_type=MESH)
        pl.semaphore_wait(barrier, len(peers))

        def block(n, i, h=None):
            if h is None:
                return full.at[n, rows(i)]
            return full.at[n, pl.ds(pl.multiple_of(i * R + h * (R // 2), R // 2), R // 2)]

        def send_own():
            for n in (1, 0):
                loads[n].wait()
                for d in SIDES:
                    mine = block(n, y)
                    send(mine, mine, full_sem.at[n, d, 0], (z, x, c, turn(y, d)))

        def send_help():
            loads[2].wait()
            for d in (1, 3, 0):
                device = (z, x, 1 - c, turn(y, d))
                send(help_rows.at[0], block(2, y), full_sem.at[2, d, 0], device)
            loads[3].wait()
            send(help_rows.at[1], last, last_sem, (z, x, 1 - c, y))

        def pass_on(n):
            for d, h in ((1, 0), (3, 1)):
                i = back(y, d)
                arrive(block(n, i), full_sem.at[n, d, 0], (z, x, c, i))
                mine = block(n, i, h)
                send(mine, mine, full_sem.at[n, 2, h], (z, x, c, turn(y, d)))

        def await_far(n):
            for h in (0, 1):
                i = back(y, 2)
                arrive(block(n, i, h), full_sem.at[n, 2, h], (z, x, c, i))

        def drive():
            loads[4].wait()
            loads[5].wait()
            first = 2 * c
            for l in range(2):
                stage[first + l] = row_dot([(gain[l], seen[l : l + 1])])
            mine = stage.at[first : first + 2]
            if forward:
                drives[y, 0:2] = stage[0:2]
            for d in (1, 3, 2) if forward else (0, 1, 3, 2):
                target = drives.at[y, first : first + 2]
                send(mine, target, drive_sem.at[c, d], (z, x, 0, turn(y, d)))

        def await_drives():
            for cc in (0, 1):
                for d in (1, 3, 2) if cc == 0 else (0, 1, 3, 2):
                    i = back(y, d)
                    target = drives.at[i, 2 * cc : 2 * cc + 2]
                    arrive(target, drive_sem.at[cc, d], (z, x, cc, i))

        def compose():
            for n in (2, 1, 0):
                pass_on(n)
            if forward:
                send_help()
            arrive(block(2, y), full_sem.at[2, 0, 0], (z, x, 1 - c, y))
            arrive(last, last_sem, (z, x, 1 - c, y))
            await_far(2)
            tails[0] = mat(last[...], full[2])
            await_far(1)
            tails[1] = mat(tails[0], full[1])
            if forward:
                await_drives()
                share_shift()
            await_far(0)
            whole = mat(tails[1], full[0])
            @pl.when(lax.rem(place, 2) == 0)
            def _():
                for k in range(B):
                    columns[place, y, k] = cut(whole, k)

            @pl.when(lax.rem(place, 2) == 1)
            def _():
                for k in range(B):
                    columns[place, y, k] = cut(whole, k).T

        def piece(dp, d, k):
            return columns.at[back(place, dp), back(y, d), k[0] : k[1]]

        def to_y(dp, d, k, e):
            mine = piece(dp, d, k)
            send(mine, mine, column_sem.at[dp, (d + e) % B, k[0]], (z, x, c, turn(y, e)))

        def to_x(dp, d, k, e):
            mine = piece(dp, d, k)
            device = (z, x_at(turn(place, e)), c, y)
            send(mine, mine, column_sem.at[(dp + e) % B, d, k[0]], device)

        def got(dp, d, k):
            arrive(piece(dp, d, k), column_sem.at[dp, d, k[0]], (z, x, c, back(y, 1)))

        def share_columns():
            for to, k in ((to_y, YX), (to_x, XY), (to_x, YX), (to_y, XY)):
                for e in SIDES:
                    to(0, 0, k, e)

        def finish_prefixes():
            @pl.when(lax.rem(place, 2) == 0)
            def _():
                for k in range(B):
                    prefix[3, k] = columns[place, y, k].T

            @pl.when(lax.rem(place, 2) == 1)
            def _():
                for k in range(B):
                    prefix[3, k] = columns[place, y, k]

            tails[2] = mat(full[2, rows(y)], full[1])
            both = mat(jnp.concatenate([full[1, rows(y)], tails[2]], axis=0), full[0])
            first, second = both[:R], both[R:]
            zeroth = full[0, rows(y)]
            for k in range(B):
                prefix[0, k] = cut(zeroth, k).T
                prefix[1, k] = cut(first, k).T
                prefix[2, k] = cut(second, k).T

        def relay(d):
            for e in SIDES:
                got(e, d, YX)
                to_x(e, d, YX_PART[e], e)
                got(d, e, XY)
                to_y(d, e, XY_PART[e], e)

        def forward_columns():
            for e in SIDES:
                got(0, e, YX)
                to_y(0, e, YX_PART[e], e)
                got(e, 0, XY)
                to_x(e, 0, XY_PART[e], e)
            if forward:
                spread_shift()
            for d in SIDES:
                for e in SIDES:
                    to_x(0, d, YX, e)
                    to_y(d, 0, XY, e)
            relay(0)
            for e in SIDES:
                got(0, 2, YX_PART[e])
                got(2, 0, XY_PART[e])
            for e in (1, 3, 2):
                to_x(0, 2, YX, e)
                to_y(2, 0, XY, e)
            for d in (1, 3):
                relay(d)
            for e in SIDES:
                got(e, 2, YX)
                got(2, e, XY)

        def await_columns():
            for d in (0, 1, 3):
                for e in SIDES:
                    got(2, d, YX_PART[e])
                    got(d, 2, XY_PART[e])
            got(2, 2, YX)
            got(2, 2, XY)

        def pairs(rows_of_map, i):
            return [(cut(rows_of_map, k), drives[k, i]) for k in range(B)]

        def share_shift():
            parts = pairs(tails[1], 0) + pairs(tails[0], 1) + pairs(last[...], 2)
            shift = row_dot(parts) + drives[y, 3]
            shifts[place, y] = shift
            mine = shifts.at[place, y]
            for e in (1, 3, 2):
                send(mine, mine, shift_y_sem.at[e], (z, x, c, turn(y, e)))

        def spread_shift():
            for e in (1, 3, 2):
                i = back(y, e)
                arrive(shifts.at[place, i], shift_y_sem.at[e], (z, x, c, i))
            mine = shifts.at[place]
            for e in (1, 3, 2):
                send(mine, mine, shift_x_sem.at[e], (z, x_at(turn(place, e)), c, y))

        def other_offsets():
            third = row_dot(pairs(tails[2], 0) + pairs(full[2, rows(y)], 1))
            offsets[2] = third + drives[y, 2]
            offsets[1] = row_dot(pairs(full[1, rows(y)], 0)) + drives[y, 1]
            offsets[0] = drives[y, 0]

        def await_shifts():
            if forward:
                for e in (1, 3, 2):
                    p = back(place, e)
                    arrive(shifts.at[p], shift_x_sem.at[e], (z, x_at(p), c, y))
            else:
                for e in range(B):
                    p = back(place, e)
                    for d in range(B):
                        i = back(y, d)
                        arrive(shifts.at[p, i], back_shift_sem.at[e, d], (z, x_at(p), 0, i))
            for n in range(2):
                for k in range(B):
                    shift_spread[n, k] = spread(shifts[2 * n, k])

        def pair(n, state):
            for i in range(B):
                total = None
                for k in range(B):
                    term = columns[2 * n, i, k] * state[k]
                    total = term if total is None else total + term
                reduced = jnp.sum(total, axis=1, keepdims=True)
                spreads[2 * n + 1, i] = jnp.broadcast_to(reduced, (R, R)) + shift_spread[n, i]
            result = []
            for i in range(B):
                total = None
                for k in range(B):
                    term = fold(columns[2 * n + 1, i, k] * spreads[2 * n + 1, k])
                    total = term if total is None else total + term
                result.append(jnp.sum(total, axis=0, keepdims=True) + shifts[2 * n + 1, i])
            return result

        def open_gate():
            device = (z, x, 1, y)
            pl.semaphore_signal(gate_sem, inc=1, device_id=device, device_id_type=MESH)

        def expand():
            def row_of(n, k):
                return spreads[n, k].T[0:1]

            ends = (
                lambda k: entering[k],
                lambda k: row_of(1, k),
                lambda k: middle[k],
                lambda k: row_of(3, k),
                lambda k: leaving[k],
            )
            for n in range(B):

                @pl.when(place == n)
                def _():
                    for k in range(B):
                        first[k] = ends[n](k)
                        states[k, 3] = ends[n + 1](k)

            row = [first[k] for k in range(B)]
            for i in range(3):
                maps = [full[i, k * R : (k + 1) * R] for k in range(B)]
                row = [
                    row_dot([(cut(a, j), row[j]) for j in range(B)]) + drives[k, i]
                    for k, a in enumerate(maps)
                ]
                for k in range(B):
                    states[k, i] = row[k]

        def column_rows():
            @pl.when(place == 0)
            def _():
                for k in range(B):
                    spreads[0, k] = spread(entering[k])

            @pl.when(place == 2)
            def _():
                for k in range(B):
                    spreads[2, k] = spread(middle[k])

            @pl.when(level == 0)
            def _():
                back_offsets()

            for i in range(4):
                total = None
                for k in range(B):
                    term = fold(prefix[i, k] * spreads[place, k])
                    total = term if total is None else total + term
                rows_out[i] = jnp.sum(total, axis=0, keepdims=True) + offsets[i]

        def back_offsets():
            arrive(drives, drives_sem, (z, x, 0, y))
            other_offsets()
            offsets[3] = shifts[place, y]

        def chain():
            up, down = (z + 1, z - 1) if forward else (z - 1, z + 1)

            @pl.when(level == 0)
            def _():
                entering[...] = start[...]

            @pl.when(level > 0)
            def _():
                if not forward:
                    back_offsets()
                arrive(entering, hop_sem, (down, x, c, y))

            state = pair(0, [entering[k] for k in range(B)])
            for k in range(B):
                middle[k] = state[k]
            state = pair(1, state)
            for k in range(B):
                leaving[k] = state[k]
            hop = remote(leaving, entering, hop_sem, (up, x, c, y))

            @pl.when(level < Z - 1)
            def _():
                hop.start()

            if forward:
                expand()
            else:
                column_rows()

            @pl.when(level < Z - 1)
            def _():
                hop.wait_send()

            sends.append(None)

        def share_states():
            send(states.at[y, 2:4], filtered_in, filtered_sem, (z, x, 1, y))
            for l in range(2):
                filtered_out[l : l + 1] = states[y, l]

        def pull():
            loads[6].wait()
            arrive(pull_map.at[2:4], pull_sem, (z, x, 1, y))
            for i in range(4):
                step = pull_map[3 - i]
                pulled[y, i] = row_dot([(cut(step, k), states[k, 3 - i]) for k in range(B)])
            mine = pulled.at[y]
            for d in (1, 3, 2):
                send(mine, mine, pulled_sem.at[d], (z, x, 0, turn(y, d)))
            arrive(back_tails, tails_sem, (z, x, 1, y))
            for d in (1, 3, 2):
                i = back(y, d)
                arrive(pulled.at[i], pulled_sem.at[d], (z, x, 0, i))
            maps = (back_tails[1], back_tails[0], help_rows[1])
            parts = [(cut(a, k), pulled[k, i]) for i, a in enumerate(maps) for k in range(B)]
            back_shift[...] = row_dot(parts) + pulled[y, 3]
            p = B - 1 - x
            for e in range(B):
                for d in range(B):
                    device = (z, B - 1 - turn(p, e), 1, turn(y, d))
                    send(back_shift, shifts.at[p, y], back_shift_sem.at[e, d], device)
            send(pulled, drives, drives_sem, (z, x, 1, y))

        if forward:
            send_own()
            drive()
            compose()
            share_columns()
            forward_columns()
            open_gate()
            await_shifts()
            await_columns()
            loads[7].wait()
            chain()
            pull()
            share_states()
            arrive(smoothed_in, smoothed_sem, (z, x, 1, y))
            for l in range(2):
                smoothed_out[l : l + 1] = smoothed_in[1 - l]
        else:
            send_help()
            drive()
            loads[6].wait()
            send(pull_map.at[2:4], pull_map.at[2:4], pull_sem, (z, x, 0, y))
            pl.semaphore_wait(gate_sem, 1)
            send_own()
            compose()
            send(tails.at[0:2], back_tails, tails_sem, (z, x, 0, y))
            share_columns()
            finish_prefixes()
            forward_columns()
            await_shifts()
            await_columns()
            loads[7].wait()
            chain()
            send(rows_out.at[2:4], smoothed_in, smoothed_sem, (z, x, 0, y))
            arrive(filtered_in, filtered_sem, (z, x, 0, y))
            for l in range(2):
                filtered_out[l : l + 1] = filtered_in[l]
                smoothed_out[l : l + 1] = rows_out[1 - l]
        for copy in sends:
            if copy is not None:
                copy.wait_send()

    @pl.when(core == 0)
    def _():
        branch(0)

    @pl.when(core == 1)
    def _():
        branch(1)


def shards(prior_mean, after_mean, filter_map, smoother_gain, smoother_map, obs_gain, observations):
    f32 = jnp.float32
    n = B * R
    vmem = pl.BlockSpec(memory_space=pltpu.VMEM)
    hbm = pl.BlockSpec(memory_space=pltpu.HBM)
    dma = pltpu.SemaphoreType.DMA
    shapes = [
        (3, n, n), (R, n), (2, R, n), (4, R, n), (2, R, R), (3, R, n),
        (4, B, R, R), (4, B, B, R, R), (4, B, R, R), (2, B, R, R),
        (4, B, 1, R), (4, 1, R), (B, 4, 1, R), (4, 1, R),
        (B, 1, R), (B, 1, R), (B, 1, R), (4, 1, R), (B, 4, 1, R), (2, 1, R), (2, R), (B, 1, R),
        (2, R, n), (B, 4, 1, R), (1, R), (2, 1, R), (B, 1, R),
    ]
    both = pl.pallas_call(
        kernel,
        out_shape=jax.ShapeDtypeStruct((2, 2, R), f32),
        in_specs=[hbm] * 7,
        out_specs=vmem,
        scratch_shapes=[pltpu.VMEM(shape, f32) for shape in shapes]
        + [
            dma((8,)), dma((96,)), dma((3, B, 2)), dma, dma((2, B)), dma((B, B, 4)),
            dma((B,)), dma((B,)), dma, dma, pltpu.SemaphoreType.REGULAR,
            dma, dma, dma((B,)), dma, dma((B, B)), dma,
        ],
        compiler_params=pltpu.CompilerParams(
            collective_id=0, has_side_effects=True, vmem_limit_bytes=VMEM_LIMIT
        ),
        name="smoother",
    )(
        prior_mean.reshape(B, 1, R),
        after_mean.reshape(B, 1, R),
        filter_map,
        smoother_gain,
        smoother_map,
        obs_gain,
        observations,
    )
    return both[0], both[1]


def solution(mesh):
    torus = Mesh(mesh.devices.reshape(8, 4, 2, mesh.shape["blk"]), (*TM, "blk"))
    in_specs = (
        P(),
        P(),
        P(TM, "blk", None),
        P(TM, "blk", None),
        P(TM, "blk", None),
        P(TM, "blk", None),
        P(TM, None),
    )
    out_specs = (P(TM, "blk"), P(TM, "blk"))
    return jax.shard_map(
        shards, mesh=torus, in_specs=in_specs, out_specs=out_specs, check_vma=False
    )
```

```python
import functools

import jax
import jax.numpy as jnp
from jax import lax
from jax.experimental import pallas as pl
from jax.experimental.pallas import tpu as pltpu
from jax.sharding import Mesh
from jax.sharding import PartitionSpec as P

TM = ("tm_0", "tm_1", "tm_2")
MESH = pl.DeviceIdType.MESH
R = 128
B = 4
Z = 8
SIDES = (1, 3)
YX, XY = (0, 2), (2, 4)
FAR = sorted(((e, d) for e in range(B) for d in range(B)), key=lambda o: sum(min(i, B - i) for i in o))
YX_PART, XY_PART = {1: (0, 1), 3: (1, 2)}, {1: (2, 3), 3: (3, 4)}
VMEM_LIMIT = 67_043_328


def mat(a, b):
    high, low = [], []
    for value in (a, b):
        top = value.astype(jnp.bfloat16)
        high.append(top)
        low.append((value - top.astype(jnp.float32)).astype(jnp.bfloat16))
    dot = functools.partial(jnp.dot, preferred_element_type=jnp.float32)
    return dot(high[0], high[1]) + (dot(high[0], low[1]) + dot(low[0], high[1]))


def spread(row):
    return jnp.broadcast_to(row, (R, R)).T


def row_dot(pairs):
    total = None
    for a, u in pairs:
        total = a * u if total is None else total + a * u
    return jnp.sum(total.T, axis=0, keepdims=True)


def fold(product):
    return jnp.sum(product.reshape(R // 8, 8, R), axis=0)


def cut(block, k):
    return block[:, k * R : (k + 1) * R]


def kernel(
    prior,
    after,
    filter_map,
    smoother_gain,
    smoother_map,
    obs_gain,
    observations,
    both_out,
    full,
    last,
    help_rows,
    pull_map,
    gain,
    tails,
    prefix,
    columns,
    spreads,
    shift_spread,
    shifts,
    stage,
    drives,
    offsets,
    entering,
    middle,
    leaving,
    rows_out,
    states,
    smoothed_in,
    seen,
    start,
    back_tails,
    pulled,
    back_shift,
    filtered_in,
    first,
    load_sem,
    send_sem,
    full_sem,
    last_sem,
    drive_sem,
    column_sem,
    shift_y_sem,
    shift_x_sem,
    hop_sem,
    smoothed_sem,
    gate_sem,
    pull_sem,
    tails_sem,
    pulled_sem,
    drives_sem,
    back_shift_sem,
    filtered_sem,
):
    filtered_out, smoothed_out = both_out.at[0], both_out.at[1]
    z, x, y = lax.axis_index("tm_0"), lax.axis_index("tm_1"), lax.axis_index("blk")
    core = lax.axis_index("tm_2")

    def branch(c):
        forward = c == 0
        own = filter_map if forward else smoother_gain
        other = smoother_gain if forward else filter_map
        place = x if forward else B - 1 - x
        level = z if forward else Z - 1 - z
        sends = []

        def x_at(p):
            return p if forward else B - 1 - p

        def turn(i, d):
            return lax.rem(i + d, B)

        def back(i, d):
            return lax.rem(i + B - d, B)

        def rows(i):
            return pl.ds(pl.multiple_of(i * R, R), R)

        def remote(src, dst, recv, device):
            return pltpu.make_async_remote_copy(
                src_ref=src,
                dst_ref=dst,
                send_sem=send_sem.at[len(sends)],
                recv_sem=recv,
                device_id=device,
                device_id_type=MESH,
            )

        def send(src, dst, recv, device):
            copy = remote(src, dst, recv, device)
            copy.start()
            sends.append(copy)

        def arrive(dst, recv, device):
            pltpu.make_async_remote_copy(
                src_ref=dst,
                dst_ref=dst,
                send_sem=send_sem.at[0],
                recv_sem=recv,
                device_id=device,
                device_id_type=MESH,
            ).wait_recv()

        loads = []

        def load(src, dst):
            copy = pltpu.make_async_copy(src, dst, load_sem.at[len(loads)])
            copy.start()
            loads.append(copy)

        load(own.at[c], full.at[0, rows(y)])
        load(own.at[1 - c], full.at[1, rows(y)])
        load(other.at[1 - c], help_rows.at[0])
        load(other.at[c], help_rows.at[1])
        load(obs_gain, gain)
        load(observations, seen)
        load(smoother_map, pull_map.at[2 * c : 2 * c + 2])
        load(prior if forward else after, start)

        barrier = pltpu.get_barrier_semaphore()
        peers = [(z, x, c, turn(y, d)) for d in (1, 2, 3)]
        peers += [(z, turn(x, d), c, y) for d in (1, 2, 3)]
        peers += [(lax.rem(z + 1, Z), x, c, y), (lax.rem(z + Z - 1, Z), x, c, y)]
        peers += [(z, turn(x, e), 1 - c, turn(y, d)) for e in range(B) for d in range(B)]
        for peer in peers:
            pl.semaphore_signal(barrier, inc=1, device_id=peer, device_id_type=MESH)
        pl.semaphore_wait(barrier, len(peers))

        def block(n, i, h=None):
            if h is None:
                return full.at[n, rows(i)]
            return full.at[n, pl.ds(pl.multiple_of(i * R + h * (R // 2), R // 2), R // 2)]

        def send_own():
            for n in (1, 0):
                loads[n].wait()
                for d in SIDES:
                    mine = block(n, y)
                    send(mine, mine, full_sem.at[n, d, 0], (z, x, c, turn(y, d)))

        def send_help():
            loads[2].wait()
            for d in (1, 3, 0):
                device = (z, x, 1 - c, turn(y, d))
                send(help_rows.at[0], block(2, y), full_sem.at[2, d, 0], device)
            loads[3].wait()
            send(help_rows.at[1], last, last_sem, (z, x, 1 - c, y))

        def pass_on(n):
            for d, h in ((1, 0), (3, 1)):
                i = back(y, d)
                arrive(block(n, i), full_sem.at[n, d, 0], (z, x, c, i))
                mine = block(n, i, h)
                send(mine, mine, full_sem.at[n, 2, h], (z, x, c, turn(y, d)))

        def await_far(n):
            for h in (0, 1):
                i = back(y, 2)
                arrive(block(n, i, h), full_sem.at[n, 2, h], (z, x, c, i))

        def drive():
            loads[4].wait()
            loads[5].wait()
            first = 2 * c
            for l in range(2):
                stage[first + l] = row_dot([(gain[l], seen[l : l + 1])])
            mine = stage.at[first : first + 2]
            if forward:
                drives[y, 0:2] = stage[0:2]
            for d in (1, 3, 2) if forward else (0, 1, 3, 2):
                target = drives.at[y, first : first + 2]
                send(mine, target, drive_sem.at[c, d], (z, x, 0, turn(y, d)))

        def await_drives():
            for cc in (0, 1):
                for d in (1, 3, 2) if cc == 0 else (0, 1, 3, 2):
                    i = back(y, d)
                    target = drives.at[i, 2 * cc : 2 * cc + 2]
                    arrive(target, drive_sem.at[cc, d], (z, x, cc, i))

        def compose():
            for n in (2, 1, 0):
                pass_on(n)
            if forward:
                send_help()
            arrive(block(2, y), full_sem.at[2, 0, 0], (z, x, 1 - c, y))
            arrive(last, last_sem, (z, x, 1 - c, y))
            await_far(2)
            tails[0] = mat(last[...], full[2])
            await_far(1)
            tails[1] = mat(tails[0], full[1])
            if forward:
                await_drives()
                share_shift()
            await_far(0)
            whole = mat(tails[1], full[0])
            @pl.when(lax.rem(place, 2) == 0)
            def _():
                for k in range(B):
                    columns[place, y, k] = cut(whole, k)

            @pl.when(lax.rem(place, 2) == 1)
            def _():
                for k in range(B):
                    columns[place, y, k] = cut(whole, k).T

        def piece(dp, d, k):
            return columns.at[back(place, dp), back(y, d), k[0] : k[1]]

        def to_y(dp, d, k, e):
            mine = piece(dp, d, k)
            send(mine, mine, column_sem.at[dp, (d + e) % B, k[0]], (z, x, c, turn(y, e)))

        def to_x(dp, d, k, e):
            mine = piece(dp, d, k)
            device = (z, x_at(turn(place, e)), c, y)
            send(mine, mine, column_sem.at[(dp + e) % B, d, k[0]], device)

        def got(dp, d, k):
            arrive(piece(dp, d, k), column_sem.at[dp, d, k[0]], (z, x, c, back(y, 1)))

        def share_columns():
            for to, k in ((to_y, YX), (to_x, XY), (to_x, YX), (to_y, XY)):
                for e in SIDES:
                    to(0, 0, k, e)

        def finish_prefixes():
            @pl.when(lax.rem(place, 2) == 0)
            def _():
                for k in range(B):
                    prefix[3, k] = columns[place, y, k].T

            @pl.when(lax.rem(place, 2) == 1)
            def _():
                for k in range(B):
                    prefix[3, k] = columns[place, y, k]

            tails[2] = mat(full[2, rows(y)], full[1])
            both = mat(jnp.concatenate([full[1, rows(y)], tails[2]], axis=0), full[0])
            first, second = both[:R], both[R:]
            zeroth = full[0, rows(y)]
            for k in range(B):
                prefix[0, k] = cut(zeroth, k).T
                prefix[1, k] = cut(first, k).T
                prefix[2, k] = cut(second, k).T

        def relay(d):
            for e in SIDES:
                got(e, d, YX)
                to_x(e, d, YX_PART[e], e)
                got(d, e, XY)
                to_y(d, e, XY_PART[e], e)

        def forward_columns():
            for e in SIDES:
                got(0, e, YX)
                to_y(0, e, YX_PART[e], e)
                got(e, 0, XY)
                to_x(e, 0, XY_PART[e], e)
            if forward:
                spread_shift()
            for d in SIDES:
                for e in SIDES:
                    to_x(0, d, YX, e)
                    to_y(d, 0, XY, e)
            relay(0)
            for e in SIDES:
                got(0, 2, YX_PART[e])
                got(2, 0, XY_PART[e])
            for e in (1, 3, 2):
                to_x(0, 2, YX, e)
                to_y(2, 0, XY, e)
            for d in (1, 3):
                relay(d)
            for e in SIDES:
                got(e, 2, YX)
                got(2, e, XY)

        def await_columns():
            for d in (0, 1, 3):
                for e in SIDES:
                    got(2, d, YX_PART[e])
                    got(d, 2, XY_PART[e])
            got(2, 2, YX)
            got(2, 2, XY)

        def pairs(rows_of_map, i):
            return [(cut(rows_of_map, k), drives[k, i]) for k in range(B)]

        def share_shift():
            parts = pairs(tails[1], 0) + pairs(tails[0], 1) + pairs(last[...], 2)
            shift = row_dot(parts) + drives[y, 3]
            shifts[place, y] = shift
            mine = shifts.at[place, y]
            for e in (1, 3, 2):
                send(mine, mine, shift_y_sem.at[e], (z, x, c, turn(y, e)))

        def spread_shift():
            for e in (1, 3, 2):
                i = back(y, e)
                arrive(shifts.at[place, i], shift_y_sem.at[e], (z, x, c, i))
            mine = shifts.at[place]
            for e in (1, 3, 2):
                send(mine, mine, shift_x_sem.at[e], (z, x_at(turn(place, e)), c, y))

        def other_offsets():
            third = row_dot(pairs(tails[2], 0) + pairs(full[2, rows(y)], 1))
            offsets[2] = third + drives[y, 2]
            offsets[1] = row_dot(pairs(full[1, rows(y)], 0)) + drives[y, 1]
            offsets[0] = drives[y, 0]

        def await_shifts():
            if forward:
                for e in (1, 3, 2):
                    p = back(place, e)
                    arrive(shifts.at[p], shift_x_sem.at[e], (z, x_at(p), c, y))
                for n in range(2):
                    for k in range(B):
                        shift_spread[n, k] = spread(shifts[2 * n, k])
            else:
                for e, d in FAR:
                    p, i = back(place, e), back(y, d)
                    arrive(shifts.at[p, i], back_shift_sem.at[e, d], (z, x_at(p), 0, i))

                    @pl.when(lax.rem(p, 2) == 0)
                    def _():
                        shift_spread[lax.div(p, 2), i] = spread(shifts[p, i])

        def pair(n, state):
            for i in range(B):
                total = None
                for k in range(B):
                    term = columns[2 * n, i, k] * state[k]
                    total = term if total is None else total + term
                reduced = jnp.sum(total, axis=1, keepdims=True)
                spreads[2 * n + 1, i] = jnp.broadcast_to(reduced, (R, R)) + shift_spread[n, i]
            result = []
            for i in range(B):
                total = None
                for k in range(B):
                    term = fold(columns[2 * n + 1, i, k] * spreads[2 * n + 1, k])
                    total = term if total is None else total + term
                result.append(jnp.sum(total, axis=0, keepdims=True) + shifts[2 * n + 1, i])
            return result

        def open_gate():
            device = (z, x, 1, y)
            pl.semaphore_signal(gate_sem, inc=1, device_id=device, device_id_type=MESH)

        def expand():
            def row_of(n, k):
                return spreads[n, k].T[0:1]

            ends = (
                lambda k: entering[k],
                lambda k: row_of(1, k),
                lambda k: middle[k],
                lambda k: row_of(3, k),
                lambda k: leaving[k],
            )
            for n in range(B):

                @pl.when(place == n)
                def _():
                    for k in range(B):
                        first[k] = ends[n](k)
                        states[k, 3] = ends[n + 1](k)

            row = [first[k] for k in range(B)]
            for i in range(3):
                maps = [full[i, k * R : (k + 1) * R] for k in range(B)]
                row = [
                    row_dot([(cut(a, j), row[j]) for j in range(B)]) + drives[k, i]
                    for k, a in enumerate(maps)
                ]
                for k in range(B):
                    states[k, i] = row[k]

        def column_rows():
            @pl.when(place == 0)
            def _():
                for k in range(B):
                    spreads[0, k] = spread(entering[k])

            @pl.when(place == 2)
            def _():
                for k in range(B):
                    spreads[2, k] = spread(middle[k])

            @pl.when(level == 0)
            def _():
                back_offsets()

            for i in range(4):
                total = None
                for k in range(B):
                    term = fold(prefix[i, k] * spreads[place, k])
                    total = term if total is None else total + term
                rows_out[i] = jnp.sum(total, axis=0, keepdims=True) + offsets[i]

        def back_offsets():
            arrive(drives, drives_sem, (z, x, 0, y))
            other_offsets()
            offsets[3] = shifts[place, y]

        def chain():
            up, down = (z + 1, z - 1) if forward else (z - 1, z + 1)

            @pl.when(level == 0)
            def _():
                entering[...] = start[...]

            @pl.when(level > 0)
            def _():
                if not forward:
                    back_offsets()
                arrive(entering, hop_sem, (down, x, c, y))

            state = pair(0, [entering[k] for k in range(B)])
            for k in range(B):
                middle[k] = state[k]
            state = pair(1, state)
            for k in range(B):
                leaving[k] = state[k]
            hop = remote(leaving, entering, hop_sem, (up, x, c, y))

            @pl.when(level < Z - 1)
            def _():
                hop.start()

            if forward:
                expand()
            else:
                column_rows()

            @pl.when(level < Z - 1)
            def _():
                hop.wait_send()

            sends.append(None)

        def share_states():
            send(states.at[y, 2:4], filtered_in, filtered_sem, (z, x, 1, y))
            for l in range(2):
                filtered_out[l : l + 1] = states[y, l]

        def pull():
            loads[6].wait()
            arrive(pull_map.at[2:4], pull_sem, (z, x, 1, y))
            for i in range(4):
                step = pull_map[3 - i]
                pulled[y, i] = row_dot([(cut(step, k), states[k, 3 - i]) for k in range(B)])
            mine = pulled.at[y]
            for d in (2, 1, 3):
                send(mine, mine, pulled_sem.at[d], (z, x, 0, turn(y, d)))
            arrive(back_tails, tails_sem, (z, x, 1, y))
            for d in (1, 3, 2):
                i = back(y, d)
                arrive(pulled.at[i], pulled_sem.at[d], (z, x, 0, i))
            maps = (back_tails[1], back_tails[0], help_rows[1])
            parts = [(cut(a, k), pulled[k, i]) for i, a in enumerate(maps) for k in range(B)]
            back_shift[...] = row_dot(parts) + pulled[y, 3]
            p = B - 1 - x
            for e, d in FAR[::-1]:
                device = (z, B - 1 - turn(p, e), 1, turn(y, d))
                send(back_shift, shifts.at[p, y], back_shift_sem.at[e, d], device)
            send(pulled, drives, drives_sem, (z, x, 1, y))

        if forward:
            send_own()
            drive()
            compose()
            share_columns()
            forward_columns()
            await_shifts()
            await_columns()
            open_gate()
            loads[7].wait()
            chain()
            pull()
            share_states()
            arrive(smoothed_in, smoothed_sem, (z, x, 1, y))
            for l in range(2):
                smoothed_out[l : l + 1] = smoothed_in[1 - l]
        else:
            send_help()
            drive()
            loads[6].wait()
            send(pull_map.at[2:4], pull_map.at[2:4], pull_sem, (z, x, 0, y))
            pl.semaphore_wait(gate_sem, 1)
            send_own()
            compose()
            share_columns()
            send(tails.at[0:2], back_tails, tails_sem, (z, x, 0, y))
            forward_columns()
            finish_prefixes()
            await_shifts()
            await_columns()
            loads[7].wait()
            chain()
            send(rows_out.at[2:4], smoothed_in, smoothed_sem, (z, x, 0, y))
            arrive(filtered_in, filtered_sem, (z, x, 0, y))
            for l in range(2):
                filtered_out[l : l + 1] = filtered_in[l]
                smoothed_out[l : l + 1] = rows_out[1 - l]
        for copy in sends:
            if copy is not None:
                copy.wait_send()

    @pl.when(core == 0)
    def _():
        branch(0)

    @pl.when(core == 1)
    def _():
        branch(1)


def shards(prior_mean, after_mean, filter_map, smoother_gain, smoother_map, obs_gain, observations):
    f32 = jnp.float32
    n = B * R
    vmem = pl.BlockSpec(memory_space=pltpu.VMEM)
    hbm = pl.BlockSpec(memory_space=pltpu.HBM)
    dma = pltpu.SemaphoreType.DMA
    shapes = [
        (3, n, n), (R, n), (2, R, n), (4, R, n), (2, R, R), (3, R, n),
        (4, B, R, R), (4, B, B, R, R), (4, B, R, R), (2, B, R, R),
        (4, B, 1, R), (4, 1, R), (B, 4, 1, R), (4, 1, R),
        (B, 1, R), (B, 1, R), (B, 1, R), (4, 1, R), (B, 4, 1, R), (2, 1, R), (2, R), (B, 1, R),
        (2, R, n), (B, 4, 1, R), (1, R), (2, 1, R), (B, 1, R),
    ]
    both = pl.pallas_call(
        kernel,
        out_shape=jax.ShapeDtypeStruct((2, 2, R), f32),
        in_specs=[hbm] * 7,
        out_specs=vmem,
        scratch_shapes=[pltpu.VMEM(shape, f32) for shape in shapes]
        + [
            dma((8,)), dma((96,)), dma((3, B, 2)), dma, dma((2, B)), dma((B, B, 4)),
            dma((B,)), dma((B,)), dma, dma, pltpu.SemaphoreType.REGULAR,
            dma, dma, dma((B,)), dma, dma((B, B)), dma,
        ],
        compiler_params=pltpu.CompilerParams(
            collective_id=0, has_side_effects=True, vmem_limit_bytes=VMEM_LIMIT
        ),
        name="smoother",
    )(
        prior_mean.reshape(B, 1, R),
        after_mean.reshape(B, 1, R),
        filter_map,
        smoother_gain,
        smoother_map,
        obs_gain,
        observations,
    )
    return both[0], both[1]


def solution(mesh):
    torus = Mesh(mesh.devices.reshape(8, 4, 2, mesh.shape["blk"]), (*TM, "blk"))
    in_specs = (
        P(),
        P(),
        P(TM, "blk", None),
        P(TM, "blk", None),
        P(TM, "blk", None),
        P(TM, "blk", None),
        P(TM, None),
    )
    out_specs = (P(TM, "blk"), P(TM, "blk"))
    return jax.shard_map(
        shards, mesh=torus, in_specs=in_specs, out_specs=out_specs, check_vma=False
    )
```
